16 devices in a mesh: sp: 16 (over z, y, x, core).
Axes of the slice: x: 2, y: 2, z: 2, core: 2. Of those that a mesh axis runs over, the one named last changes fastest.
Arguments:
- hidden: bfloat16 [16, 1024, 2048], P(None, 'sp')
- d_out: bfloat16 [16, 1024, 2048], P(None, 'sp')
- w_query: bfloat16 [2048, 16, 128], replicated
- w_key: bfloat16 [2048, 128], replicated
- w_value: bfloat16 [2048, 128], replicated
- w_out: bfloat16 [16, 128, 2048], replicated
Outputs:
- output 1: bfloat16 [16, 1024, 2048], P(None, 'sp')
- output 2: bfloat16 [16, 1024, 2048], P(None, 'sp')
- output 3: float32 [2048, 16, 128], replicated
- output 4: float32 [2048, 128], replicated
- output 5: float32 [2048, 128], replicated
- output 6: float32 [16, 128, 2048], replicated
All inputs are finite; a program needn't handle non-finite values.
Results may differ from the reference program's by a relative error of at most 0.0196.
Values are sent between devices in bfloat16 or wider.
A program may use at most 1 GiB of HBM per device.

```python
import jax
import jax.numpy as jnp
from jax import lax

BATCH_SIZE = 16
SEQ_LEN = 1024
MODEL_DIM = 2048
NUM_HEADS = 16
HEAD_DIM = 128

HALF_DIM = HEAD_DIM // 2
SCORE_SCALE = HEAD_DIM ** -0.5


def setup_inputs(seed: int = 0) -> dict:
    keys = jax.random.split(jax.random.key(seed), 6)
    act_shape = (BATCH_SIZE, SEQ_LEN, MODEL_DIM)
    hidden = jax.random.normal(keys[0], act_shape, jnp.float32)
    d_out = jax.random.normal(keys[1], act_shape, jnp.float32)
    w_query = jax.random.normal(keys[2], (MODEL_DIM, NUM_HEADS, HEAD_DIM), jnp.float32) * MODEL_DIM ** -0.5
    w_key = jax.random.normal(keys[3], (MODEL_DIM, HEAD_DIM), jnp.float32) * MODEL_DIM ** -0.5
    w_value = jax.random.normal(keys[4], (MODEL_DIM, HEAD_DIM), jnp.float32) * MODEL_DIM ** -0.5
    w_out = jax.random.normal(keys[5], (NUM_HEADS, HEAD_DIM, MODEL_DIM), jnp.float32) * (NUM_HEADS * HEAD_DIM) ** -0.5
    return {'hidden': hidden.astype(jnp.bfloat16), 'd_out': d_out.astype(jnp.bfloat16), 'w_query': w_query.astype(jnp.bfloat16), 'w_key': w_key.astype(jnp.bfloat16), 'w_value': w_value.astype(jnp.bfloat16), 'w_out': w_out.astype(jnp.bfloat16)}


def rope_tables(positions):
    inv_freq = 10000.0 ** (-(jnp.arange(HALF_DIM).astype(jnp.float32) * 2.0) / HEAD_DIM)
    angles = positions.astype(jnp.float32)[:, None] * inv_freq[None, :]
    return jnp.cos(angles), jnp.sin(angles)


def rotate(values, cos_tab, sin_tab):
    lead_half, tail_half = values[..., :HALF_DIM], values[..., HALF_DIM:]
    return jnp.concatenate([lead_half * cos_tab - tail_half * sin_tab, tail_half * cos_tab + lead_half * sin_tab], axis=-1)


def rotate_back(cotangent, cos_tab, sin_tab):
    lead_half, tail_half = cotangent[..., :HALF_DIM], cotangent[..., HALF_DIM:]
    return jnp.concatenate([lead_half * cos_tab + tail_half * sin_tab, tail_half * cos_tab - lead_half * sin_tab], axis=-1)


def causal_softmax(scores):
    row_max = jnp.max(scores, axis=-1, keepdims=True)
    expo_vals = jnp.exp(scores - row_max)
    return expo_vals / jnp.sum(expo_vals, axis=-1, keepdims=True)


def reference(hidden, d_out, w_query, w_key, w_value, w_out):
    cos_tab, sin_tab = rope_tables(jnp.arange(SEQ_LEN))
    hidden_wide = hidden.astype(jnp.float32)
    q_proj = jnp.einsum('bld,dhe->blhe', hidden_wide, w_query.astype(jnp.float32)).astype(jnp.bfloat16)
    k_proj = jnp.einsum('bld,de->ble', hidden_wide, w_key.astype(jnp.float32)).astype(jnp.bfloat16)
    v_proj = jnp.einsum('bld,de->ble', hidden_wide, w_value.astype(jnp.float32)).astype(jnp.bfloat16)
    q_rot = rotate(q_proj.astype(jnp.float32), cos_tab[:, None, :], sin_tab[:, None, :]).astype(jnp.bfloat16)
    k_rot = rotate(k_proj.astype(jnp.float32), cos_tab, sin_tab).astype(jnp.bfloat16)
    k_wide = k_rot.astype(jnp.float32)
    v_wide = v_proj.astype(jnp.float32)
    causal = jnp.arange(SEQ_LEN)[:, None] >= jnp.arange(SEQ_LEN)[None, :]

    def head_probs(q_head):
        scores = jnp.einsum('bqe,bke->bqk', q_head.astype(jnp.float32), k_wide) * SCORE_SCALE
        return causal_softmax(jnp.where(causal, scores, -jnp.inf))

    def head_forward(q_head):
        attn_prob = head_probs(q_head)
        return jnp.einsum('bqk,bke->bqe', attn_prob.astype(jnp.bfloat16).astype(jnp.float32), v_wide).astype(jnp.bfloat16)

    q_heads = jnp.moveaxis(q_rot, 2, 0)
    attn = lax.map(head_forward, q_heads)
    attn_wide = attn.astype(jnp.float32)
    w_out_wide = w_out.astype(jnp.float32)
    attn_out = jnp.einsum('hble,hed->bld', attn_wide, w_out_wide).astype(jnp.bfloat16)
    d_out_wide = d_out.astype(jnp.float32)
    d_attn = jnp.einsum('bld,hed->hble', d_out_wide, w_out_wide).astype(jnp.bfloat16)

    def head_backward(acc_pair, head_slices):
        q_head, attn_head, d_head = head_slices
        attn_prob = head_probs(q_head)
        d_head_wide = d_head.astype(jnp.float32)
        d_prob = jnp.einsum('bqe,bke->bqk', d_head_wide, v_wide)
        row_delta = jnp.sum(d_head_wide * attn_head.astype(jnp.float32), axis=-1, keepdims=True)
        d_scores = (attn_prob * (d_prob - row_delta) * SCORE_SCALE).astype(jnp.bfloat16).astype(jnp.float32)
        dq_head = jnp.einsum('bqk,bke->bqe', d_scores, k_wide).astype(jnp.bfloat16)
        dk_acc = acc_pair[0] + jnp.einsum('bqk,bqe->bke', d_scores, q_head.astype(jnp.float32))
        dv_acc = acc_pair[1] + jnp.einsum('bqk,bqe->bke', attn_prob.astype(jnp.bfloat16).astype(jnp.float32), d_head_wide)
        return (dk_acc, dv_acc), dq_head

    zero_acc = jnp.zeros((BATCH_SIZE, SEQ_LEN, HEAD_DIM), jnp.float32)
    (dk_sum, dv_sum), dq_heads = lax.scan(head_backward, (zero_acc, zero_acc), (q_heads, attn, d_attn))
    d_query = rotate_back(jnp.moveaxis(dq_heads, 0, 2).astype(jnp.float32), cos_tab[:, None, :], sin_tab[:, None, :]).astype(jnp.bfloat16)
    d_key = rotate_back(dk_sum.astype(jnp.bfloat16).astype(jnp.float32), cos_tab, sin_tab).astype(jnp.bfloat16)
    d_value = dv_sum.astype(jnp.bfloat16)
    dq_wide = d_query.astype(jnp.float32)
    dk_wide = d_key.astype(jnp.float32)
    dv_wide = d_value.astype(jnp.float32)
    d_hidden = (jnp.einsum('blhe,dhe->bld', dq_wide, w_query.astype(jnp.float32)) + jnp.einsum('ble,de->bld', dk_wide, w_key.astype(jnp.float32)) + jnp.einsum('ble,de->bld', dv_wide, w_value.astype(jnp.float32))).astype(jnp.bfloat16)
    grad_w_query = jnp.einsum('bld,blhe->dhe', hidden_wide, dq_wide)
    grad_w_key = jnp.einsum('bld,ble->de', hidden_wide, dk_wide)
    grad_w_value = jnp.einsum('bld,ble->de', hidden_wide, dv_wide)
    grad_w_out = jnp.einsum('hble,bld->hed', attn_wide, d_out_wide)
    return (attn_out, d_hidden, grad_w_query, grad_w_key, grad_w_value, grad_w_out)
```

```python
import functools

import jax
import jax.numpy as jnp
from jax import lax
from jax.experimental import pallas as pl
from jax.experimental.pallas import tpu as pltpu
from jax.sharding import PartitionSpec as P

F32 = jnp.float32
BF16 = jnp.bfloat16
LOG2E = 1.4426950408889634
NT = (((1,), (1,)), ((), ()))
TN = (((0,), (0,)), ((), ()))


def rope_tables(positions, head_dim):
    half_dim = head_dim // 2
    inv_freq = 10000.0 ** (-(jnp.arange(half_dim).astype(F32) * 2.0) / head_dim)
    angles = positions.astype(F32)[:, None] * inv_freq[None, :]
    return jnp.cos(angles), jnp.sin(angles)


def rotate(values, cos_tab, sin_tab):
    half_dim = values.shape[-1] // 2
    lead_half, tail_half = values[..., :half_dim], values[..., half_dim:]
    return jnp.concatenate([lead_half * cos_tab - tail_half * sin_tab, tail_half * cos_tab + lead_half * sin_tab], axis=-1)


def rotate_back(cotangent, cos_tab, sin_tab):
    half_dim = cotangent.shape[-1] // 2
    lead_half, tail_half = cotangent[..., :half_dim], cotangent[..., half_dim:]
    return jnp.concatenate([lead_half * cos_tab + tail_half * sin_tab, tail_half * cos_tab - lead_half * sin_tab], axis=-1)


def attn_kernel(n_tiles, scale, q_ref, do_ref, kv_ref, cos_ref, sin_ref, cap_ref, o_ref, dq_ref, dkv_ref, dk_acc, dv_acc):
    heads, length, dim = q_ref.shape
    ndev = kv_ref.shape[0]
    keys = ndev * length
    k = kv_ref[:, 0, 0].reshape(keys, dim)
    v = kv_ref[:, 1, 0].reshape(keys, dim)
    hpt = heads // n_tiles
    rows = hpt * length
    cosd = cos_ref[...][None]
    sind = sin_ref[...][None]
    for t in range(n_tiles):
        hs = pl.ds(t * hpt, hpt)
        qf = q_ref[hs].astype(F32)
        qr = (qf * cosd + pltpu.roll(qf, dim // 2, 2) * sind).astype(BF16).reshape(rows, dim)
        s = lax.dot_general(qr, k, NT, preferred_element_type=F32)
        s = jnp.minimum(s.reshape(hpt, length, keys), cap_ref[...][None]).reshape(rows, keys)
        m = jnp.max(s, axis=1, keepdims=True)
        e = jnp.exp2((s - m) * (scale * LOG2E))
        p = e * (1.0 / jnp.sum(e, axis=1, keepdims=True))
        pb = p.astype(BF16)
        ob = lax.dot(pb, v, preferred_element_type=F32).astype(BF16)
        o_ref[hs] = ob.reshape(hpt, length, dim)
        do = do_ref[hs].reshape(rows, dim)
        delta = jnp.sum(do.astype(F32) * ob.astype(F32), axis=1, keepdims=True)
        dp = lax.dot_general(do, v, NT, preferred_element_type=F32)
        ds = (p * (dp - delta) * scale).astype(BF16)
        dqr = lax.dot(ds, k, preferred_element_type=F32).astype(BF16).astype(F32).reshape(hpt, length, dim)
        dq_ref[hs] = (dqr * cosd - pltpu.roll(dqr, dim // 2, 2) * sind).astype(BF16)
        dv = lax.dot_general(pb, do, TN, preferred_element_type=F32)
        dk = lax.dot_general(ds, qr, TN, preferred_element_type=F32)
        if t == 0:
            dk_acc[...] = dk
            dv_acc[...] = dv
        elif t < n_tiles - 1:
            dk_acc[...] += dk
            dv_acc[...] += dv
        else:
            dkv_ref[:, 0, 0] = (dk_acc[...] + dk).reshape(ndev, length, dim)
            dkv_ref[:, 1, 0] = (dv_acc[...] + dv).reshape(ndev, length, dim)


def attention(q, do, kv_all, cos_tab, sin_tab, cap, scale):
    heads, tokens, dim = q.shape
    ndev, _, batch, length, _ = kv_all.shape
    keys = ndev * length
    rows_spec = pl.BlockSpec((heads, length, dim), lambda b: (0, b, 0))
    kv_spec = pl.BlockSpec((ndev, 2, 1, length, dim), lambda b: (0, 0, b, 0, 0))
    flops = 12 * batch * heads * length * keys * dim
    return pl.pallas_call(
        functools.partial(attn_kernel, 4, scale),
        grid=(batch,),
        in_specs=[rows_spec, rows_spec, kv_spec,
                  pl.BlockSpec((length, dim), lambda b: (0, 0)),
                  pl.BlockSpec((length, dim), lambda b: (0, 0)),
                  pl.BlockSpec((length, keys), lambda b: (0, 0))],
        out_specs=[rows_spec, rows_spec, kv_spec],
        out_shape=[jax.ShapeDtypeStruct(q.shape, BF16), jax.ShapeDtypeStruct(q.shape, BF16),
                   jax.ShapeDtypeStruct(kv_all.shape, F32)],
        scratch_shapes=[pltpu.VMEM((keys, dim), F32), pltpu.VMEM((keys, dim), F32)],
        compiler_params=pltpu.CompilerParams(vmem_limit_bytes=48 * 1024 * 1024),
        cost_estimate=pl.CostEstimate(flops=flops, bytes_accessed=40 * 1024 * 1024, transcendentals=batch * heads * length * keys),
        name="attn",
    )(q, do, kv_all, cos_tab, sin_tab, cap)


def solution(mesh):
    axis_size = mesh.shape['sp']
    seq_spec = P(None, 'sp', None)
    rep_spec = P()

    def local_step(hidden, d_out, w_query, w_key, w_value, w_out):
        batch, local_len, width = hidden.shape
        head_dim = w_key.shape[1]
        seq_len = local_len * axis_size
        tokens = batch * local_len
        score_scale = head_dim ** -0.5
        positions = lax.axis_index('sp') * local_len + jnp.arange(local_len)
        cos_tab, sin_tab = rope_tables(positions, head_dim)
        cos_full = jnp.concatenate([cos_tab, cos_tab], axis=-1)
        sin_full = jnp.concatenate([-sin_tab, sin_tab], axis=-1)
        cap = jnp.where(positions[:, None] >= jnp.arange(seq_len)[None, :], jnp.inf, -jnp.inf).astype(F32)
        hid = hidden.reshape(tokens, width)
        dout = d_out.reshape(tokens, width)
        k_proj = jnp.einsum('bld,de->ble', hidden, w_key, preferred_element_type=F32).astype(BF16)
        v_proj = jnp.einsum('bld,de->ble', hidden, w_value, preferred_element_type=F32).astype(BF16)
        k_rot = rotate(k_proj.astype(F32), cos_tab, sin_tab).astype(BF16)
        kv_all = lax.all_gather(jnp.stack([k_rot, v_proj]), 'sp')
        q = jnp.einsum('td,dhe->hte', hid, w_query, preferred_element_type=F32).astype(BF16)
        do = jnp.einsum('td,hed->hte', dout, w_out, preferred_element_type=F32).astype(BF16)
        o, dq, dkv = attention(q, do, kv_all, cos_full, sin_full, cap, score_scale)
        grad_w_out = lax.psum(jnp.einsum('hte,td->hed', o, dout, preferred_element_type=F32), 'sp')
        grad_w_query = lax.psum(jnp.einsum('td,hte->dhe', hid, dq, preferred_element_type=F32), 'sp')
        kv_grad = lax.psum_scatter(dkv, 'sp', scatter_dimension=0, tiled=False).astype(BF16)
        attn_out = jnp.einsum('hte,hed->td', o, w_out, preferred_element_type=F32).astype(BF16).reshape(hidden.shape)
        d_key = rotate_back(kv_grad[0].astype(F32), cos_tab, sin_tab).astype(BF16)
        d_value = kv_grad[1]
        d_hidden = (jnp.einsum('hte,dhe->td', dq, w_query, preferred_element_type=F32).reshape(hidden.shape) + jnp.einsum('ble,de->bld', d_key, w_key, preferred_element_type=F32) + jnp.einsum('ble,de->bld', d_value, w_value, preferred_element_type=F32)).astype(BF16)
        grad_w_key = jnp.einsum('bld,ble->de', hidden, d_key, preferred_element_type=F32)
        grad_w_value = jnp.einsum('bld,ble->de', hidden, d_value, preferred_element_type=F32)
        grad_w_key, grad_w_value = lax.psum((grad_w_key, grad_w_value), 'sp')
        return (attn_out, d_hidden, grad_w_query, grad_w_key, grad_w_value, grad_w_out)

    return jax.shard_map(local_step, mesh=mesh, in_specs=(seq_spec, seq_spec, rep_spec, rep_spec, rep_spec, rep_spec), out_specs=(seq_spec, seq_spec, rep_spec, rep_spec, rep_spec, rep_spec), check_vma=False)
```

```python
import functools

import jax
import jax.numpy as jnp
from jax import lax
from jax.experimental import pallas as pl
from jax.experimental.pallas import tpu as pltpu
from jax.sharding import PartitionSpec as P

F32 = jnp.float32
BF16 = jnp.bfloat16
LOG2E = 1.4426950408889634
NT = (((1,), (1,)), ((), ()))
TN = (((0,), (0,)), ((), ()))


def rope_tables(positions, head_dim):
    half_dim = head_dim // 2
    inv_freq = 10000.0 ** (-(jnp.arange(half_dim).astype(F32) * 2.0) / head_dim)
    angles = positions.astype(F32)[:, None] * inv_freq[None, :]
    return jnp.cos(angles), jnp.sin(angles)


def rotate(values, cos_tab, sin_tab):
    half_dim = values.shape[-1] // 2
    lead_half, tail_half = values[..., :half_dim], values[..., half_dim:]
    return jnp.concatenate([lead_half * cos_tab - tail_half * sin_tab, tail_half * cos_tab + lead_half * sin_tab], axis=-1)


def rotate_back(cotangent, cos_tab, sin_tab):
    half_dim = cotangent.shape[-1] // 2
    lead_half, tail_half = cotangent[..., :half_dim], cotangent[..., half_dim:]
    return jnp.concatenate([lead_half * cos_tab + tail_half * sin_tab, tail_half * cos_tab - lead_half * sin_tab], axis=-1)


def attn_kernel(n_tiles, scale, q_ref, do_ref, kv_ref, cos_ref, sin_ref, cap_ref, o_ref, dq_ref, dkv_ref, dk_acc, dv_acc):
    heads, length, dim = q_ref.shape
    ndev = kv_ref.shape[0]
    keys = ndev * length
    k = kv_ref[:, 0, 0].reshape(keys, dim)
    v = kv_ref[:, 1, 0].reshape(keys, dim)
    hpt = heads // n_tiles
    rows = hpt * length
    cosd = cos_ref[...][None]
    sind = sin_ref[...][None]
    for t in range(n_tiles):
        hs = pl.ds(t * hpt, hpt)
        qf = q_ref[hs].astype(F32)
        qr = (qf * cosd + pltpu.roll(qf, dim // 2, 2) * sind).astype(BF16).reshape(rows, dim)
        s = lax.dot_general(qr, k, NT, preferred_element_type=F32)
        s = jnp.minimum(s.reshape(hpt, length, keys), cap_ref[...][None]).reshape(rows, keys)
        m = jnp.max(s, axis=1, keepdims=True)
        e = jnp.exp2((s - m) * (scale * LOG2E))
        p = e * (1.0 / jnp.sum(e, axis=1, keepdims=True))
        pb = p.astype(BF16)
        ob = lax.dot(pb, v, preferred_element_type=F32).astype(BF16)
        o_ref[hs] = ob.reshape(hpt, length, dim)
        do = do_ref[hs].reshape(rows, dim)
        delta = jnp.sum(do.astype(F32) * ob.astype(F32), axis=1, keepdims=True)
        dp = lax.dot_general(do, v, NT, preferred_element_type=F32)
        ds = (p * (dp - delta) * scale).astype(BF16)
        dqr = lax.dot(ds, k, preferred_element_type=F32).astype(BF16).astype(F32).reshape(hpt, length, dim)
        dq_ref[hs] = (dqr * cosd - pltpu.roll(dqr, dim // 2, 2) * sind).astype(BF16)
        dv = lax.dot_general(pb, do, TN, preferred_element_type=F32)
        dk = lax.dot_general(ds, qr, TN, preferred_element_type=F32)
        if t == 0:
            dk_acc[...] = dk
            dv_acc[...] = dv
        elif t < n_tiles - 1:
            dk_acc[...] += dk
            dv_acc[...] += dv
        else:
            dkv_ref[:, 0, 0] = (dk_acc[...] + dk).reshape(ndev, length, dim)
            dkv_ref[:, 1, 0] = (dv_acc[...] + dv).reshape(ndev, length, dim)


def attention(q, do, kv_all, cos_tab, sin_tab, cap, scale):
    heads, tokens, dim = q.shape
    ndev, _, batch, length, _ = kv_all.shape
    keys = ndev * length
    rows_spec = pl.BlockSpec((heads, length, dim), lambda b: (0, b, 0))
    kv_spec = pl.BlockSpec((ndev, 2, 1, length, dim), lambda b: (0, 0, b, 0, 0))
    flops = 12 * batch * heads * length * keys * dim
    return pl.pallas_call(
        functools.partial(attn_kernel, 4, scale),
        grid=(batch,),
        in_specs=[rows_spec, rows_spec, kv_spec,
                  pl.BlockSpec((length, dim), lambda b: (0, 0)),
                  pl.BlockSpec((length, dim), lambda b: (0, 0)),
                  pl.BlockSpec((length, keys), lambda b: (0, 0))],
        out_specs=[rows_spec, rows_spec, kv_spec],
        out_shape=[jax.ShapeDtypeStruct(q.shape, BF16), jax.ShapeDtypeStruct(q.shape, BF16),
                   jax.ShapeDtypeStruct(kv_all.shape, F32)],
        scratch_shapes=[pltpu.VMEM((keys, dim), F32), pltpu.VMEM((keys, dim), F32)],
        compiler_params=pltpu.CompilerParams(vmem_limit_bytes=48 * 1024 * 1024),
        cost_estimate=pl.CostEstimate(flops=flops, bytes_accessed=40 * 1024 * 1024, transcendentals=batch * heads * length * keys),
        name="attn",
    )(q, do, kv_all, cos_tab, sin_tab, cap)


MESH = pl.DeviceIdType.MESH
COLORS = ((1, 2, 4), (2, 4, 1), (4, 1, 2))
ORDER = (7, 3, 6, 5, 1, 2, 4, 0)


class Place:
    def __init__(self):
        me = lax.axis_index('sp')
        self.core = me % 2
        self.bits = ((me // 2) % 2, (me // 4) % 2, me // 8)

    def chip(self, rel):
        x, y, z = [1 - b if rel >> i & 1 else b for i, b in enumerate(self.bits)]
        return z * 4 + y * 2 + x

    def device(self, rel, other_core=False):
        return self.chip(rel) * 2 + (1 - self.core if other_core else self.core)


class Copies:
    def __init__(self, send_sem, recv_sem):
        self.send_sem, self.recv_sem = send_sem, recv_sem
        self.started, self.n = [], 0

    def remote(self, src, dst, device):
        copy = pltpu.make_async_remote_copy(src_ref=src, dst_ref=dst, send_sem=self.send_sem.at[self.n], recv_sem=self.recv_sem.at[self.n],
                                            device_id=(device,), device_id_type=MESH)
        self.n += 1
        copy.start()
        self.started.append(copy.wait_send)
        return copy

    def local(self, src, dst):
        copy = pltpu.make_async_copy(src, dst, self.send_sem.at[self.n])
        self.n += 1
        copy.start()
        return copy

    def finish(self):
        for wait in self.started:
            wait()


def entry_barrier(place):
    barrier = pltpu.get_barrier_semaphore()
    for device in (place.device(0, True), place.device(1), place.device(2), place.device(4)):
        pl.semaphore_signal(barrier, inc=1, device_id=(device,), device_id_type=MESH)
    pl.semaphore_wait(barrier, 4)


def add_into(dst, src):
    dst[...] += src[...]


class Halving:
    def __init__(self, place, copies, own, r1, r2, r3):
        self.place, self.copies, self.own = place, copies, own
        self.recv = (r1, r2, r3)
        self.arrive = {}

    def slots(self, color, stage):
        m1, m2, m3 = COLORS[color]
        return ((m2, m2 | m3, m3, 0), (m3, 0), (0,))[stage]

    def send(self, rel, color, stage):
        mask = COLORS[color][stage]
        landed = rel ^ mask
        slot = self.slots(color, stage).index(landed)
        dst = self.recv[stage].at[slot, self.part(color)]
        self.arrive[(stage, color, landed)] = (self.copies.remote(self.own(rel, color), dst, self.place.device(mask)), dst)

    def part(self, color):
        return self.parts[color]

    def ready(self, rel):
        for color in range(3):
            if rel & COLORS[color][0]:
                self.send(rel, color, 0)

    def run(self):
        for stage in range(3):
            for i in range((4, 2, 1)[stage]):
                for color in range(3):
                    rel = self.slots(color, stage)[i]
                    copy, landed = self.arrive[(stage, color, rel)]
                    copy.wait_recv()
                    add_into(self.own(rel, color), landed)
                    if stage < 2 and rel & COLORS[color][stage + 1]:
                        self.send(rel, color, stage + 1)


def kv_reduce_kernel(parts, x_ref, out_ref, acc, recv0, r1, r2, r3, send_sem, recv_sem):
    place = Place()
    copies = Copies(send_sem, recv_sem)
    entry_barrier(place)
    loads, d2d = {}, {}
    for rel in ORDER:
        d2d[rel] = copies.remote(x_ref.at[place.device(rel, True)], recv0.at[rel], place.device(0, True))
        loads[rel] = copies.local(x_ref.at[place.device(rel)], acc.at[rel])
    halving = Halving(place, copies, lambda rel, color: acc.at[rel, parts[color]], r1, r2, r3)
    halving.parts = parts
    for rel in ORDER:
        loads[rel].wait()
        d2d[rel].wait_recv()
        add_into(acc.at[rel], recv0.at[rel])
        halving.ready(rel)
    halving.run()
    out_ref[...] = acc[0].astype(BF16)
    copies.finish()


def kv_reduce(x):
    ndev, slabs, rows, dim = x.shape
    third = -(-slabs // 3)
    parts = tuple(pl.ds(c * third, min(third, slabs - c * third)) for c in range(3))
    buf = lambda n: pltpu.VMEM((n, slabs, rows, dim), F32)
    return pl.pallas_call(
        functools.partial(kv_reduce_kernel, parts),
        out_shape=jax.ShapeDtypeStruct((slabs, rows, dim), BF16),
        in_specs=[pl.BlockSpec(memory_space=pl.ANY)],
        out_specs=pl.BlockSpec(memory_space=pltpu.VMEM),
        scratch_shapes=[buf(8), buf(8), buf(4), buf(2), buf(1), pltpu.SemaphoreType.DMA((40,)), pltpu.SemaphoreType.DMA((40,))],
        compiler_params=pltpu.CompilerParams(collective_id=0, has_side_effects=True, vmem_limit_bytes=48 * 1024 * 1024),
        cost_estimate=pl.CostEstimate(flops=1_000_000, bytes_accessed=32 * 1024 * 1024, transcendentals=0),
        name="kv_reduce",
    )(x)


def weight_grads_kernel(hid_ref, dq_ref, dkv_ref, out_ref, x, recv0, r1, r2, r3, gat, send_sem, recv_sem):
    place = Place()
    core = place.core
    copies = Copies(send_sem, recv_sem)
    entry_barrier(place)
    heads, tokens, dim = dq_ref.shape
    slabs = x.shape[2]
    wide, small = dim, dim // heads
    parts = tuple(pl.ds(c * (slabs // 3), slabs // 3) for c in range(3))
    halving = Halving(place, copies, lambda rel, color: x.at[rel, core, parts[color]], r1, r2, r3)
    halving.parts = parts

    def partial_block(rel):
        cols = pl.ds(pl.multiple_of(place.chip(rel) * 2 * dim, 2 * dim), 2 * dim)
        hid_t = hid_ref[:, cols].T
        for pair in range(heads // 2):
            rhs = jnp.concatenate([dq_ref[2 * pair], dq_ref[2 * pair + 1]], axis=1)
            g = jnp.dot(hid_t, rhs, preferred_element_type=F32)
            for i in range(2):
                for h in range(2):
                    x[rel, i, 0:wide, 2 * pair + h, :] = g[i * dim:(i + 1) * dim, h * dim:(h + 1) * dim]
        g = jnp.dot(hid_t, dkv_ref[...], preferred_element_type=F32)
        for i in range(2):
            for h in range(2):
                x[rel, i, wide + h * small:wide + (h + 1) * small] = g[i * dim:(i + 1) * dim, h * dim:(h + 1) * dim].reshape(small, heads, dim)

    d2d = {}

    def paired(rel):
        d2d[rel].wait_recv()
        add_into(x.at[rel, core], recv0.at[rel])
        halving.ready(rel)

    last = None
    for rel in ORDER:
        partial_block(rel)
        d2d[rel] = copies.remote(x.at[rel, 1 - core], recv0.at[rel], place.device(0, True))
        if last is not None:
            paired(last)
        last = rel
    paired(last)
    halving.run()

    arrive, tail = {}, []

    def have(rel, color, src):
        m1, m2, m3 = COLORS[color]
        masks = (m3, m2, m1) if rel == 0 else (m2, m1) if rel == m3 else (m1,) if rel in (m2, m2 | m3) else ()
        for mask in masks:
            landed = rel | mask
            dst = gat.at[landed, parts[color]]
            arrive[(color, landed)] = (copies.remote(src, dst, place.device(mask)), dst)
        home = out_ref.at[place.device(rel), parts[color]]
        tail.append(copies.local(src, home).wait)
        tail.append(copies.remote(src, home, place.device(0, True)).wait_recv)

    for color in range(3):
        have(0, color, x.at[0, core, parts[color]])
    for step in range(7):
        for color in range(3):
            m1, m2, m3 = COLORS[color]
            rel = (m3, m2, m1, m2 | m3, m1 | m3, m1 | m2, 7)[step]
            copy, landed = arrive[(color, rel)]
            copy.wait_recv()
            have(rel, color, landed)
    for wait in tail:
        wait()
    copies.finish()


def weight_grads(hid, dq, dkv):
    heads, tokens, dim = dq.shape
    slabs = dim + 2 * (dim // heads)
    buf = lambda *n: pltpu.VMEM((*n, slabs, heads, dim), F32)
    vmem = pl.BlockSpec(memory_space=pltpu.VMEM)
    return pl.pallas_call(
        weight_grads_kernel,
        out_shape=jax.ShapeDtypeStruct((16, slabs, heads, dim), F32),
        in_specs=[vmem, vmem, vmem],
        out_specs=pl.BlockSpec(memory_space=pl.ANY),
        scratch_shapes=[buf(8, 2), buf(8), buf(4), buf(2), buf(1), buf(8), pltpu.SemaphoreType.DMA((128,)), pltpu.SemaphoreType.DMA((128,))],
        compiler_params=pltpu.CompilerParams(collective_id=1, has_side_effects=True, vmem_limit_bytes=63 * 1024 * 1024),
        cost_estimate=pl.CostEstimate(flops=1_000_000, bytes_accessed=64 * 1024 * 1024, transcendentals=0),
        name="weight_grads",
    )(hid, dq, dkv)


def solution(mesh):
    axis_size = mesh.shape['sp']
    seq_spec = P(None, 'sp', None)
    rep_spec = P()

    def local_step(hidden, d_out, w_query, w_key, w_value, w_out):
        batch, local_len, width = hidden.shape
        head_dim = w_key.shape[1]
        num_heads = w_query.shape[1]
        seq_len = local_len * axis_size
        tokens = batch * local_len
        score_scale = head_dim ** -0.5
        positions = lax.axis_index('sp') * local_len + jnp.arange(local_len)
        cos_tab, sin_tab = rope_tables(positions, head_dim)
        cos_full = jnp.concatenate([cos_tab, cos_tab], axis=-1)
        sin_full = jnp.concatenate([-sin_tab, sin_tab], axis=-1)
        cap = jnp.where(positions[:, None] >= jnp.arange(seq_len)[None, :], jnp.inf, -jnp.inf).astype(F32)
        hid = hidden.reshape(tokens, width)
        dout = d_out.reshape(tokens, width)
        k_proj = jnp.einsum('bld,de->ble', hidden, w_key, preferred_element_type=F32).astype(BF16)
        v_proj = jnp.einsum('bld,de->ble', hidden, w_value, preferred_element_type=F32).astype(BF16)
        k_rot = rotate(k_proj.astype(F32), cos_tab, sin_tab).astype(BF16)
        kv_all = lax.all_gather(jnp.stack([k_rot, v_proj]), 'sp')
        q = jnp.einsum('td,dhe->hte', hid, w_query, preferred_element_type=F32).astype(BF16)
        do = jnp.einsum('td,hed->hte', dout, w_out, preferred_element_type=F32).astype(BF16)
        o, dq, dkv = attention(q, do, kv_all, cos_full, sin_full, cap, score_scale)
        grad_out_part, dkv = lax.optimization_barrier((jnp.einsum('hte,td->hed', o, dout, preferred_element_type=F32), dkv))
        grad_w_out = lax.psum(grad_out_part, 'sp')
        kv_grad = kv_reduce(dkv.reshape(axis_size, 2 * batch, local_len, head_dim)).reshape(2, batch, local_len, head_dim)
        d_key = rotate_back(kv_grad[0].astype(F32), cos_tab, sin_tab).astype(BF16)
        d_value = kv_grad[1]
        dkv_tok = jnp.concatenate([d_key, d_value], axis=-1).reshape(tokens, 2 * head_dim)
        grads = weight_grads(hid, dq, dkv_tok)
        per = head_dim // num_heads
        grad_w_query = grads[:, :head_dim].reshape(width, num_heads, head_dim)
        grad_w_key = grads[:, head_dim:head_dim + per].reshape(width, head_dim)
        grad_w_value = grads[:, head_dim + per:].reshape(width, head_dim)
        attn_out = jnp.einsum('hte,hed->td', o, w_out, preferred_element_type=F32).astype(BF16).reshape(hidden.shape)
        d_hidden = (jnp.einsum('hte,dhe->td', dq, w_query, preferred_element_type=F32).reshape(hidden.shape) + jnp.einsum('ble,de->bld', d_key, w_key, preferred_element_type=F32) + jnp.einsum('ble,de->bld', d_value, w_value, preferred_element_type=F32)).astype(BF16)
        return (attn_out, d_hidden, grad_w_query, grad_w_key, grad_w_value, grad_w_out)

    return jax.shard_map(local_step, mesh=mesh, in_specs=(seq_spec, seq_spec, rep_spec, rep_spec, rep_spec, rep_spec), out_specs=(seq_spec, seq_spec, rep_spec, rep_spec, rep_spec, rep_spec), check_vma=False)
```
